256 devices in a mesh: section: 8 (over y_hi, x), expert: 32 (over y_lo, z, core).
Axes of the slice: x: 4, y: 4 (y_hi: 2, y_lo: 2; y = y_hi * 2 + y_lo), z: 8, core: 2. Of those that a mesh axis runs over, the one named last changes fastest.
Arguments:
- initial_batch: bfloat16 [8, 2048, 4096], P('section', 'expert'), may hold values from -6 to 6
- arriving_batches: bfloat16 [1, 2048, 4096], P(None, 'expert'), may hold values from -6 to 6
- rescaling_gains: float32 [8, 4096], P('section'), may hold values from 0.5 to 2
- gating_projection: bfloat16 [8, 4096, 14336], P('section', None, 'expert'), may hold values from -0.09375 to 0.09375
- expanding_projection: bfloat16 [8, 4096, 14336], P('section', None, 'expert'), may hold values from -0.09375 to 0.09375
- contracting_projection: bfloat16 [8, 14336, 4096], P('section', 'expert'), may hold values from -0.0625 to 0.0625
- routed_specialist_pairs: int32 [8, 2, 2048, 2], P('section', None, 'expert'), may hold values from 0 to 7, all different within a row; in each aligned block of 64 rows (0 to 63, 64 to 127, ..., all dimensions but the last counted through in order) at most 20 rows name the same one
- primary_routing_share: float32 [8, 2, 2048], P('section', None, 'expert'), may hold values from 0.1 to 0.9
Outputs:
- states: bfloat16 [8, 2, 2048, 4096], P('section', None, 'expert')
The draws below stay inside these ranges and needn't reach their ends.
Inputs may be any that keep to these rules, and one draw needn't show every extreme that they name: `routed_specialist_pairs`: A token's two ids differ. In each aligned block of 64 rows (one device's tokens at one layer and microbatch) no expert is named by more than 20 tokens.
All inputs are finite; a program needn't handle non-finite values.
Results may differ from the reference program's by a relative error of at most 0.009.
Values may be sent and summed in bfloat16 or wider, within the bound.
No kernel may reach another device: no remote copies, remote signals or barrier semaphores. Data moves between devices by JAX's collectives and lax.ppermute only.
A program may use at most 128 MiB of HBM per device.

```python
import math
import jax
import jax.numpy as jnp
import numpy as np
from jax import lax

EMBED_BREADTH = 4096
EXPERTS = 8
TOPK = 2
EXP_WIN = 2
FF_WIN = 7168
TOK_DEV = 64
TICKS = 2
GROUP = 16
HID_DEV = 448
FF_ALL = 14336
CAP = 20
BATCH_SEQ_COUNT = 2048
N_SECTION = 8
N_EXPERT = 32


def block_scale(stream_key, dims, shards, least, high):
    def one(axis_at, blocks):
        steps = jax.random.uniform(jax.random.fold_in(jax.random.fold_in(stream_key, 6), axis_at), (blocks,), jnp.float32, least / len(shards), high / len(shards))
        return jnp.repeat(jnp.exp(steps), dims[axis_at] // blocks).reshape((-1,) + (1,) * (len(dims) - axis_at - 1))

    factor_of = one(*shards[0])
    for cut in shards[1:]:
        factor_of = factor_of * one(*cut)
    return factor_of


def shared_out(own_key, own, number, rows, amount, top, limit, skew):
    order = jax.random.permutation(own_key, amount)
    packed, common = portions_of(amount, rows * top, limit, skew, True), portions_of(amount, rows * top, limit, skew, False)
    places = jnp.arange(amount)

    def named(lengths, offset_by):
        used = int((lengths > 0).sum())
        fixed = max(1, used // 4)
        shifted = fixed + (places - fixed + offset_by * (used - fixed)) % max(1, amount - fixed)
        return jnp.zeros((amount,), jnp.int32).at[order[jnp.where(places < fixed, places, shifted)]].set(jnp.asarray(lengths, jnp.int32))

    lengths = jnp.where(number % 4 == 0, named(packed, number // 4), named(common, number - number // 4 - 1))
    mixed = jax.random.permutation(jax.random.fold_in(own, 3), amount)
    donor, sink = mixed[0:amount // 2 * 2:2], mixed[1:amount // 2 * 2:2]
    slack = jnp.minimum(lengths[donor] - 1, limit - lengths[sink]) // 2
    slack = jnp.where((donor == order[0]) | (sink == order[0]) | (lengths[sink] == 0), 0, jnp.maximum(slack, 0))
    shifted = jax.random.randint(jax.random.fold_in(own, 4), (amount // 2,), 0, 1 << 20) % (slack + 1)
    lengths = lengths.at[donor].add(-shifted).at[sink].add(shifted)
    items = jnp.searchsorted(jnp.cumsum(lengths), jnp.arange(rows * top), side="right").astype(jnp.int32)
    listing = items.reshape(top, rows).T
    listing = listing[jax.random.permutation(jax.random.fold_in(own, 1), rows)]
    offset_by = jax.random.randint(jax.random.fold_in(own, 2), (rows, 1), 0, top)
    return jnp.take_along_axis(listing, (jnp.arange(top)[None, :] + offset_by) % top, axis=1)


def portions_of(number_of, total, most, skew, full):
    loads = [(1 << 20) // math.isqrt(standing ** skew) + 1 for standing in range(1, number_of + 1)]
    largest = most if full else min(most, max(-(-total // number_of), total * loads[0] // sum(loads)))
    least = 1 if total - largest >= number_of - 1 else 0
    given, surplus = [largest] + [least] * (number_of - 1), total - largest - least * (number_of - 1)
    while surplus > 0:
        candidates = [i for i in range(1, number_of) if given[i] < largest] or [i for i in range(1, number_of) if given[i] < most]
        mass, budget = sum([loads[i] for i in candidates]), surplus
        for i in candidates:
            extra = min(most - given[i], max(1, budget * loads[i] // mass), surplus)
            given[i] = given[i] + extra
            surplus = surplus - extra
    return np.array(given)


def gaussian(stream_key, dims, scale, limit, cuts=(), dtype=jnp.bfloat16):
    level = block_scale(stream_key, dims, cuts, -0.22, 0.18) if cuts else 1.0
    entries = jax.random.normal(stream_key, dims, jnp.float32) * scale * level
    return jnp.minimum(jnp.maximum(entries, -limit), limit).astype(dtype)


def setup_inputs(seed: int = 0) -> dict:
    seeds = jax.random.split(jax.random.key(seed), 9)
    initial_batch = gaussian(seeds[0], (N_SECTION, BATCH_SEQ_COUNT, EMBED_BREADTH), 1.0, 6.0, ((0, 8), (1, 32)))
    arriving_batches = gaussian(seeds[1], (TICKS - 1, BATCH_SEQ_COUNT, EMBED_BREADTH), 1.0, 6.0, ((1, 32),))
    rescaling_gains = jnp.clip(jnp.exp(math.log(2.0) - 1.3862944 * jax.random.uniform(seeds[2], (N_SECTION, EMBED_BREADTH), jnp.float32) ** block_scale(seeds[2], (N_SECTION, EMBED_BREADTH), ((0, 8),), -0.2, 0.2)), 0.5, 2.0)
    gating_projection = gaussian(seeds[3], (N_SECTION, EMBED_BREADTH, FF_ALL), EMBED_BREADTH ** -0.5, 0.09375, ((0, 8), (2, 32)))
    expanding_projection = gaussian(seeds[4], (N_SECTION, EMBED_BREADTH, FF_ALL), EMBED_BREADTH ** -0.5, 0.09375, ((0, 8), (2, 32)))
    contracting_projection = gaussian(seeds[5], (N_SECTION, FF_ALL, EMBED_BREADTH), FF_WIN ** -0.5, 0.0625, ((0, 8), (1, 32)))
    routed_specialist_pairs_keys = jax.random.split(jax.random.fold_in(seeds[6], 1), N_SECTION * TICKS * BATCH_SEQ_COUNT // TOK_DEV)
    routed_specialist_pairs_turns = jax.random.permutation(jax.random.fold_in(seeds[6], 3), N_SECTION * TICKS * BATCH_SEQ_COUNT // TOK_DEV)
    routed_specialist_pairs = jax.vmap(lambda own, number: shared_out(jax.random.fold_in(seeds[6], 2), own, number, TOK_DEV, EXPERTS, TOPK, CAP, 2))(routed_specialist_pairs_keys, routed_specialist_pairs_turns).reshape((N_SECTION, TICKS, BATCH_SEQ_COUNT, TOPK))
    primary_routing_share = jnp.clip(0.1 + 0.79999997 * jax.random.uniform(seeds[7], (N_SECTION, TICKS, BATCH_SEQ_COUNT), jnp.float32) ** block_scale(seeds[7], (N_SECTION, TICKS, BATCH_SEQ_COUNT), ((0, 8), (2, 32)), -0.2, 0.2), 0.1, 0.9)
    return {"initial_batch": initial_batch, "arriving_batches": arriving_batches, "rescaling_gains": rescaling_gains, "gating_projection": gating_projection, "expanding_projection": expanding_projection, "contracting_projection": contracting_projection, "routed_specialist_pairs": routed_specialist_pairs, "primary_routing_share": primary_routing_share}


def moe_layer(layer_input, gain, gate_cols, up_cols, down_rows, token_ids, share):
    widened = layer_input.astype(jnp.float32)
    scale = lax.rsqrt(lax.optimization_barrier(jnp.mean(widened * widened, axis=-1, keepdims=True)) + 1e-06)
    normed = (widened * scale * gain).astype(jnp.bfloat16)
    count = token_ids.shape[0]
    flat_ids = token_ids.reshape(-1).astype(jnp.int32)
    owners = (jnp.arange(2 * count) // 2).astype(jnp.int32)
    shares = jnp.stack([share, 1.0 - share], axis=-1).reshape(-1)
    width = N_EXPERT * CAP

    def per_expert(expert, total):
        order_key = jnp.where(flat_ids == expert, 0, 1) * (2 * count) + jnp.arange(2 * count)
        picked = jnp.argsort(order_key)[:width].astype(jnp.int32)
        valid = (flat_ids[picked] == expert).astype(jnp.float32)
        token_rows = normed[owners[picked]]
        start = (expert * FF_WIN).astype(jnp.int32)
        gate_part = lax.dynamic_slice_in_dim(gate_cols, start, FF_WIN, 1)
        up_part = lax.dynamic_slice_in_dim(up_cols, start, FF_WIN, 1)
        down_part = lax.dynamic_slice_in_dim(down_rows, start, FF_WIN, 0)
        gate_pre = jnp.dot(token_rows, gate_part, preferred_element_type=jnp.float32)
        up_pre = jnp.dot(token_rows, up_part, preferred_element_type=jnp.float32)
        hidden = (jax.nn.silu(gate_pre) * up_pre).astype(jnp.bfloat16)
        hidden3 = hidden.reshape(width, GROUP, HID_DEV).astype(jnp.float32)
        down3 = down_part.reshape(GROUP, HID_DEV, EMBED_BREADTH).astype(jnp.float32)
        partial_value = jnp.einsum('mgh,ghd->mgd', hidden3, down3).astype(jnp.bfloat16)
        summed = lax.optimization_barrier(jnp.sum(partial_value.astype(jnp.float32), axis=1))
        weighted = summed * (shares[picked] * valid)[:, None]
        return total.at[owners[picked]].add(weighted)
    mixture = lax.fori_loop(0, EXP_WIN, per_expert, jnp.zeros((count, EMBED_BREADTH), jnp.float32))
    mixture = mixture.astype(jnp.bfloat16)
    return (widened + mixture.astype(jnp.float32)).astype(jnp.bfloat16)

def reference(initial_batch, arriving_batches, rescaling_gains, gating_projection, expanding_projection, contracting_projection, routed_specialist_pairs, primary_routing_share):
    current_activation = [initial_batch[segment_portion] for segment_portion in range(N_SECTION)]
    results = []
    for tick in range(TICKS):
        outputs = []
        for segment_portion in range(N_SECTION):
            outputs.append(moe_layer(current_activation[segment_portion], rescaling_gains[segment_portion], gating_projection[segment_portion], expanding_projection[segment_portion], contracting_projection[segment_portion], routed_specialist_pairs[segment_portion, tick], primary_routing_share[segment_portion, tick]))
        results.append(jnp.stack(outputs))
        if tick + 1 < TICKS:
            current_activation = [arriving_batches[tick]] + outputs[:-1]
    return jnp.stack(results, axis=1)
```

```python
import jax
import jax.numpy as jnp
from jax import lax
from jax.sharding import Mesh, PartitionSpec as P

EXP_WIN = 2
TICKS = 2
CAP = 20


def routing_tables(token_ids, share, experts):
    count = token_ids.shape[0]
    flat_ids = token_ids.reshape(-1)
    member = (flat_ids[:, None] == experts[None, :]).astype(jnp.int32)
    position = jnp.cumsum(member, axis=0) - 1
    slot_index = jnp.sum(position * member, axis=1)
    which = jnp.sum(member * jnp.arange(EXP_WIN)[None, :], axis=1)
    valid = jnp.sum(member, axis=1) > 0
    target = jnp.where(valid, which * CAP + slot_index, -1)
    placed = (target[:, None] == jnp.arange(EXP_WIN * CAP)[None, :]).astype(jnp.float32)
    placed = placed.reshape(count, 2, EXP_WIN * CAP)
    dispatch_table = jnp.sum(placed, axis=1).T.astype(jnp.bfloat16)
    combine_table = placed[:, 0] * share[:, None] + placed[:, 1] * (1.0 - share)[:, None]
    return dispatch_table, combine_table


def shards(initial, arriving, gains, gate_w, up_w, down_w, pairs, shares):
    section_pos = lax.axis_index("section")
    y_pos = lax.axis_index("y")
    gain = gains[0]
    gate_cols = gate_w[0]
    up_cols = up_w[0]
    down_rows = down_w[0]
    current = initial[0]
    experts = jnp.stack([y_pos, 1 - y_pos]).astype(jnp.int32)
    swap = [(0, 1), (1, 0)]
    n_sec = lax.axis_size("section")
    fwd = [(i, i + 1) for i in range(n_sec - 1)]
    results = []
    for tick in range(TICKS):
        widened = current.astype(jnp.float32)
        scale = lax.rsqrt(jnp.mean(widened * widened, axis=-1, keepdims=True) + 1e-06)
        normed = (widened * scale * gain).astype(jnp.bfloat16)
        disp, comb = routing_tables(pairs[0, tick], shares[0, tick], experts)
        send_rows = jnp.dot(disp, normed, preferred_element_type=jnp.float32).astype(jnp.bfloat16)
        own, other = send_rows[:CAP], send_rows[CAP:]
        got = lax.ppermute(other, "y", swap)
        block = jnp.concatenate([own, got], axis=0)
        rows = lax.all_gather(block, ("z", "core"), axis=0, tiled=True)
        gate_pre = jnp.dot(rows, gate_cols, preferred_element_type=jnp.float32)
        up_pre = jnp.dot(rows, up_cols, preferred_element_type=jnp.float32)
        hidden = (jax.nn.silu(gate_pre) * up_pre).astype(jnp.bfloat16)
        partial = jnp.dot(hidden, down_rows, preferred_element_type=jnp.float32).astype(jnp.bfloat16)
        summed = lax.psum_scatter(partial, ("z", "core"), scatter_dimension=0, tiled=True)
        back = lax.ppermute(summed[CAP:], "y", swap)
        both = jnp.concatenate([summed[:CAP], back], axis=0)
        mixture = jnp.dot(comb, both.astype(jnp.float32), precision=lax.Precision.HIGHEST)
        mixture = mixture.astype(jnp.bfloat16)
        layer_out = (widened + mixture.astype(jnp.float32)).astype(jnp.bfloat16)
        results.append(layer_out)
        if tick + 1 < TICKS:
            passed = lax.ppermute(layer_out, "section", fwd)
            current = jnp.where(section_pos == 0, arriving[tick], passed)
    return jnp.stack(results)[None]


def solution(mesh):
    devices = mesh.devices
    n_sec = devices.shape[0]
    m = Mesh(devices.reshape(n_sec, 2, devices.shape[1] // 4, 2), ("section", "y", "z", "core"))
    ex = ("y", "z", "core")
    return jax.shard_map(
        shards,
        mesh=m,
        in_specs=(
            P("section", ex, None),
            P(None, ex, None),
            P("section", None),
            P("section", None, ex),
            P("section", None, ex),
            P("section", ex, None),
            P("section", None, ex, None),
            P("section", None, ex),
        ),
        out_specs=P("section", None, ex, None),
        check_vma=False,
    )
```

```python
import jax
import jax.numpy as jnp
from jax import lax
from jax.experimental import pallas as pl
from jax.experimental.pallas import tpu as pltpu
from jax.sharding import Mesh, PartitionSpec as P

EXP_WIN = 2
TICKS = 2
CAP = 20


def routing_tables(token_ids, share, experts):
    count = token_ids.shape[0]
    flat_ids = token_ids.reshape(-1)
    member = (flat_ids[:, None] == experts[None, :]).astype(jnp.int32)
    position = jnp.cumsum(member, axis=0) - 1
    slot_index = jnp.sum(position * member, axis=1)
    which = jnp.sum(member * jnp.arange(EXP_WIN)[None, :], axis=1)
    valid = jnp.sum(member, axis=1) > 0
    target = jnp.where(valid, which * CAP + slot_index, -1)
    placed = (target[:, None] == jnp.arange(EXP_WIN * CAP)[None, :]).astype(jnp.float32)
    placed = placed.reshape(count, 2, EXP_WIN * CAP)
    dispatch_table = jnp.sum(placed, axis=1).T.astype(jnp.bfloat16)
    combine_table = placed[:, 0] * share[:, None] + placed[:, 1] * (1.0 - share)[:, None]
    return dispatch_table, combine_table


def shift(x, axis, by):
    n = lax.axis_size(axis)
    return lax.ppermute(x, axis, [(i, (i + by) % n) for i in range(n)])


CUT = 24
SPLIT = 2


def ffn_kernel(rows, ga, ua, da, gb, ub, db, out, gbuf, ubuf, dbuf, hid, hid_t, gsem, usem, dsem):
    blk = gbuf.shape[1]
    units = da.shape[0]
    f32 = jnp.float32
    for i, (g, u) in enumerate(((ga, ua), (gb, ub))):
        for k in range(SPLIT):
            at = i * SPLIT + k
            pltpu.make_async_copy(g.at[pl.ds(k * blk, blk)], gbuf.at[at], gsem.at[at]).start()
            pltpu.make_async_copy(u.at[pl.ds(k * blk, blk)], ubuf.at[at], usem.at[at]).start()
    downs = [pltpu.make_async_copy(d, dbuf.at[pl.ds(i * units, units)], dsem.at[i]) for i, d in enumerate((da, db))]
    for d in downs:
        d.start()
    dims = (((1,), (1,)), ((), ()))

    def hidden_block(j, carry):
        pltpu.make_async_copy(ga.at[pl.ds(0, blk)], gbuf.at[j], gsem.at[j]).wait()
        gv = lax.dot_general(gbuf[j], rows[...], dims, preferred_element_type=f32)
        pltpu.make_async_copy(ua.at[pl.ds(0, blk)], ubuf.at[j], usem.at[j]).wait()
        uv = lax.dot_general(ubuf[j], rows[...], dims, preferred_element_type=f32)
        hid[j] = (gv / (1.0 + jnp.exp(-gv)) * uv).astype(jnp.bfloat16)
        return carry

    lax.fori_loop(0, 2 * SPLIT, hidden_block, 0)
    hid_t[...] = hid[...].reshape(2 * units, rows.shape[0]).T
    for d in downs:
        d.wait()
    cols = 1024

    def out_block(n, carry):
        at = pl.multiple_of(n * cols, cols)
        v = jnp.dot(hid_t[...], dbuf[:, pl.ds(at, cols)], preferred_element_type=f32)
        out[:, pl.ds(at, cols)] = v.astype(jnp.bfloat16)
        return carry

    lax.fori_loop(0, out.shape[1] // cols, out_block, 0)


def ffn(parts, weights):
    rows = jnp.concatenate(parts, axis=0)
    r, d = rows.shape
    (ga, ua, da), (gb, ub, db) = weights
    units = da.shape[0]
    blk = units // SPLIT
    bf16 = jnp.bfloat16
    hbm = pl.BlockSpec(memory_space=pltpu.HBM)
    return pl.pallas_call(
        ffn_kernel,
        out_shape=jax.ShapeDtypeStruct((r, d), bf16),
        in_specs=[pl.BlockSpec(memory_space=pltpu.VMEM)] + [hbm] * 6,
        out_specs=pl.BlockSpec(memory_space=pltpu.VMEM),
        scratch_shapes=[
            pltpu.VMEM((2 * SPLIT, blk, d), bf16),
            pltpu.VMEM((2 * SPLIT, blk, d), bf16),
            pltpu.VMEM((2 * units, d), bf16),
            pltpu.VMEM((2 * SPLIT, blk, r), bf16),
            pltpu.VMEM((r, 2 * units), bf16),
            pltpu.SemaphoreType.DMA((2 * SPLIT,)),
            pltpu.SemaphoreType.DMA((2 * SPLIT,)),
            pltpu.SemaphoreType.DMA((2,)),
        ],
        cost_estimate=pl.CostEstimate(flops=12 * r * d * units, transcendentals=2 * r * units,
                                      bytes_accessed=12 * units * d + 4 * r * d),
        compiler_params=pltpu.CompilerParams(vmem_limit_bytes=44 * 1024 * 1024),
        name="ffn",
    )(rows, ga, ua, da, gb, ub, db)


def mixed_experts(block, weights):
    f32, bf16 = jnp.float32, jnp.bfloat16
    half = lax.axis_size("z") // 2
    n = block.shape[0]
    up, dn = [block], [block]
    for s in range(1, half):
        up.append(shift(up[-1], "z", 1))
        dn.append(shift(dn[-1], "z", -1))
    near = [block]
    for s in range(1, half - 1):
        near += [up[s], dn[s]]
    near_part = ffn(near, weights)
    up[-1], dn[-1], near_part = lax.optimization_barrier((up[-1], dn[-1], near_part))
    far = [shift(up[-1][:CUT], "z", 1), shift(dn[-1][CUT:], "z", -1)]
    far_part = ffn([up[-1], dn[-1]] + far, weights)
    a = shift(far_part[2 * n:2 * n + CUT], "z", 1)
    b = shift(far_part[2 * n + CUT:], "z", -1)
    pd, pu = far_part[:n], far_part[n:2 * n]
    a = jnp.concatenate([(pu[:CUT].astype(f32) + a).astype(bf16), pu[CUT:]], axis=0)
    b = jnp.concatenate([pd[:CUT], (pd[CUT:].astype(f32) + b).astype(bf16)], axis=0)
    for s in range(half - 2, -1, -1):
        a, b = shift(a, "z", 1), shift(b, "z", -1)
        if s:
            at = n * (2 * s - 1)
            pd, pu = near_part[at:at + n], near_part[at + n:at + 2 * n]
            a = (pu.astype(f32) + a).astype(bf16)
            b = (pd.astype(f32) + b).astype(bf16)
    return near_part[:n].astype(f32) + a + b


def shards(initial, arriving, gains, gate_w, up_w, down_w, pairs, shares):
    section_pos = lax.axis_index("section")
    y_pos = lax.axis_index("y")
    gain = gains[0]
    mine = (gate_w[0].T, up_w[0].T, down_w[0])
    weights = (mine, tuple(shift(w, "core", 1) for w in mine))
    current = initial[0]
    experts = jnp.stack([y_pos, 1 - y_pos]).astype(jnp.int32)
    swap = [(0, 1), (1, 0)]
    n_sec = lax.axis_size("section")
    fwd = [(i, i + 1) for i in range(n_sec - 1)]
    results = []
    for tick in range(TICKS):
        widened = current.astype(jnp.float32)
        scale = lax.rsqrt(jnp.mean(widened * widened, axis=-1, keepdims=True) + 1e-06)
        normed = (widened * scale * gain).astype(jnp.bfloat16)
        disp, comb = routing_tables(pairs[0, tick], shares[0, tick], experts)
        send_rows = jnp.dot(disp, normed, preferred_element_type=jnp.float32).astype(jnp.bfloat16)
        own, other = send_rows[:CAP], send_rows[CAP:]
        got = lax.ppermute(other, "y", swap)
        block = jnp.concatenate([own, got], axis=0)
        summed = mixed_experts(block, weights).astype(jnp.bfloat16)
        back = lax.ppermute(summed[CAP:], "y", swap)
        both = jnp.concatenate([summed[:CAP], back], axis=0)
        mixture = jnp.dot(comb, both.astype(jnp.float32), precision=lax.Precision.HIGHEST)
        mixture = mixture.astype(jnp.bfloat16)
        layer_out = (widened + mixture.astype(jnp.float32)).astype(jnp.bfloat16)
        results.append(layer_out)
        if tick + 1 < TICKS:
            passed = lax.ppermute(layer_out, "section", fwd)
            current = jnp.where(section_pos == 0, arriving[tick], passed)
    return jnp.stack(results)[None]


def solution(mesh):
    devices = mesh.devices
    n_sec = devices.shape[0]
    m = Mesh(devices.reshape(n_sec, 2, devices.shape[1] // 4, 2), ("section", "y", "z", "core"))
    ex = ("y", "z", "core")
    return jax.shard_map(
        shards,
        mesh=m,
        in_specs=(
            P("section", ex, None),
            P(None, ex, None),
            P("section", None),
            P("section", None, ex),
            P("section", None, ex),
            P("section", ex, None),
            P("section", None, ex, None),
            P("section", None, ex),
        ),
        out_specs=P("section", None, ex, None),
        check_vma=False,
    )
```

```python
import functools

import jax
import jax.numpy as jnp
from jax import lax
from jax.experimental import pallas as pl
from jax.experimental.pallas import tpu as pltpu
from jax.sharding import Mesh, PartitionSpec as P

EXP_WIN = 2
TICKS = 2
CAP = 20
VMEM_MIB = 52


def routing_tables(token_ids, share, experts):
    count = token_ids.shape[0]
    flat_ids = token_ids.reshape(-1)
    member = (flat_ids[:, None] == experts[None, :]).astype(jnp.int32)
    position = jnp.cumsum(member, axis=0) - 1
    slot_index = jnp.sum(position * member, axis=1)
    which = jnp.sum(member * jnp.arange(EXP_WIN)[None, :], axis=1)
    valid = jnp.sum(member, axis=1) > 0
    target = jnp.where(valid, which * CAP + slot_index, -1)
    placed = (target[:, None] == jnp.arange(EXP_WIN * CAP)[None, :]).astype(jnp.float32)
    placed = placed.reshape(count, 2, EXP_WIN * CAP)
    dispatch_table = jnp.sum(placed, axis=1).T.astype(jnp.bfloat16)
    combine_table = placed[:, 0] * share[:, None] + placed[:, 1] * (1.0 - share)[:, None]
    return dispatch_table, combine_table


def shift(x, axis, by):
    n = lax.axis_size(axis)
    return lax.ppermute(x, axis, [(i, (i + by) % n) for i in range(n)])


SPLIT = 2
LANES = 128


def ring_shift(x, by):
    nz = lax.axis_size("z")
    pairs = [(2 * z + c, 2 * ((z + (by if c == 0 else -by)) % nz) + c) for z in range(nz) for c in range(2)]
    return lax.ppermute(x, ("z", "core"), pairs)


def ffn_kernel(*refs, count):
    chunks, (ga, ua, da, gb, ub, db, out) = refs[:count], refs[count:count + 7]
    gubuf, dbuf, x, xt, hid, hid_t, gsem, usem, dsem = refs[count + 7:]
    blk = gubuf.shape[1] // 2
    units = da.shape[0]
    f32 = jnp.float32
    r = out.shape[0]
    for i, (g, u) in enumerate(((ga, ua), (gb, ub))):
        for k in range(SPLIT):
            at = i * SPLIT + k
            pltpu.make_async_copy(g.at[pl.ds(k * blk, blk)], gubuf.at[at, pl.ds(0, blk)], gsem.at[at]).start()
            pltpu.make_async_copy(u.at[pl.ds(k * blk, blk)], gubuf.at[at, pl.ds(blk, blk)], usem.at[at]).start()
    downs = [pltpu.make_async_copy(d, dbuf.at[pl.ds(i * units, units)], dsem.at[i]) for i, d in enumerate((da, db))]
    for d in downs:
        d.start()
    at = 0
    for c in chunks:
        x[pl.ds(at, c.shape[0]), :] = c[...]
        at += c.shape[0]
    if at < x.shape[0]:
        x[pl.ds(at, x.shape[0] - at), :] = jnp.zeros((x.shape[0] - at, x.shape[1]), x.dtype)
    xt[...] = x[...].T

    def hidden_block(j, carry):
        pltpu.make_async_copy(ga.at[pl.ds(0, blk)], gubuf.at[j, pl.ds(0, blk)], gsem.at[j]).wait()
        pltpu.make_async_copy(ua.at[pl.ds(0, blk)], gubuf.at[j, pl.ds(blk, blk)], usem.at[j]).wait()
        v = jnp.dot(gubuf[j], xt[...], preferred_element_type=f32)
        gv, uv = v[:blk], v[blk:]
        hid[j] = (gv / (1.0 + jnp.exp(-gv)) * uv).astype(jnp.bfloat16)
        return carry

    lax.fori_loop(0, 2 * SPLIT, hidden_block, 0)
    hid_t[...] = hid[...].reshape(2 * units, x.shape[0]).T
    for d in downs:
        d.wait()
    cols = 1024

    def out_block(n, carry):
        at = pl.multiple_of(n * cols, cols)
        v = jnp.dot(hid_t[:r], dbuf[:, pl.ds(at, cols)], preferred_element_type=f32)
        out[:, pl.ds(at, cols)] = v.astype(jnp.bfloat16)
        return carry

    lax.fori_loop(0, out.shape[1] // cols, out_block, 0)


def ffn(chunks, weights):
    r, d = sum(c.shape[0] for c in chunks), chunks[0].shape[1]
    rp = -(-r // LANES) * LANES
    (ga, ua, da), (gb, ub, db) = weights
    units = da.shape[0]
    blk = units // SPLIT
    bf16 = jnp.bfloat16
    vmem, hbm = pl.BlockSpec(memory_space=pltpu.VMEM), pl.BlockSpec(memory_space=pltpu.HBM)
    return pl.pallas_call(
        functools.partial(ffn_kernel, count=len(chunks)),
        out_shape=jax.ShapeDtypeStruct((r, d), bf16),
        in_specs=[vmem] * len(chunks) + [hbm] * 6,
        out_specs=vmem,
        scratch_shapes=[
            pltpu.VMEM((2 * SPLIT, 2 * blk, d), bf16),
            pltpu.VMEM((2 * units, d), bf16),
            pltpu.VMEM((rp, d), bf16),
            pltpu.VMEM((d, rp), bf16),
            pltpu.VMEM((2 * SPLIT, blk, rp), bf16),
            pltpu.VMEM((rp, 2 * units), bf16),
            pltpu.SemaphoreType.DMA((2 * SPLIT,)),
            pltpu.SemaphoreType.DMA((2 * SPLIT,)),
            pltpu.SemaphoreType.DMA((2,)),
        ],
        cost_estimate=pl.CostEstimate(flops=12 * r * d * units, transcendentals=2 * r * units,
                                      bytes_accessed=12 * units * d + 4 * r * d),
        compiler_params=pltpu.CompilerParams(vmem_limit_bytes=VMEM_MIB * 1024 * 1024),
        name="ffn",
    )(*chunks, ga, ua, da, gb, ub, db)


def mixed_experts(block, weights):
    f32, bf16 = jnp.float32, jnp.bfloat16
    half = lax.axis_size("z") // 2
    n = block.shape[0]
    mine, other = [block], [shift(block, "core", 1)]
    for s in range(1, half):
        mine.append(ring_shift(mine[-1], 1))
        other.append(ring_shift(other[-1], 1))
    near = [block]
    for s in range(1, half - 1):
        near += [mine[s], other[s]]
    near_part = ffn(near, weights)
    last, near_part = lax.optimization_barrier((mine[-1], near_part))
    far_part = ffn([last, other[-1], ring_shift(last, 1)], weights)

    def part(s):
        if s == half - 1:
            return far_part[:n], far_part[n:2 * n]
        at = n * (2 * s - 1)
        return near_part[at:at + n], near_part[at + n:at + 2 * n]

    def after(x, first):
        return lax.optimization_barrier((x, first))[0]

    a, b = far_part[2 * n:], None
    for s in range(half - 1, 0, -1):
        pm, po = part(s)
        b = po if b is None else (po.astype(f32) + b).astype(bf16)
        sent, b = b, ring_shift(b, -1)
        a = after(ring_shift(a, -1), sent)
        a = (pm.astype(f32) + a).astype(bf16)
    c = shift(b, "core", 1)
    a = ring_shift(a, -1)
    return near_part[:n].astype(f32) + a + c


def shards(initial, arriving, gains, gate_w, up_w, down_w, pairs, shares):
    section_pos = lax.axis_index("section")
    y_pos = lax.axis_index("y")
    gain = gains[0]
    mine = (gate_w[0].T, up_w[0].T, down_w[0])
    weights = (mine, tuple(shift(w, "core", 1) for w in mine))
    current = initial[0]
    experts = jnp.stack([y_pos, 1 - y_pos]).astype(jnp.int32)
    swap = [(0, 1), (1, 0)]
    n_sec = lax.axis_size("section")
    fwd = [(i, i + 1) for i in range(n_sec - 1)]
    results = []
    for tick in range(TICKS):
        widened = current.astype(jnp.float32)
        scale = lax.rsqrt(jnp.mean(widened * widened, axis=-1, keepdims=True) + 1e-06)
        normed = (widened * scale * gain).astype(jnp.bfloat16)
        disp, comb = routing_tables(pairs[0, tick], shares[0, tick], experts)
        send_rows = jnp.dot(disp, normed, preferred_element_type=jnp.float32).astype(jnp.bfloat16)
        own, other = send_rows[:CAP], send_rows[CAP:]
        got = lax.ppermute(other, "y", swap)
        block = jnp.concatenate([own, got], axis=0)
        summed = mixed_experts(block, weights).astype(jnp.bfloat16)
        back = lax.ppermute(summed[CAP:], "y", swap)
        both = jnp.concatenate([summed[:CAP], back], axis=0)
        mixture = jnp.dot(comb, both.astype(jnp.float32), precision=lax.Precision.HIGHEST)
        mixture = mixture.astype(jnp.bfloat16)
        layer_out = (widened + mixture.astype(jnp.float32)).astype(jnp.bfloat16)
        results.append(layer_out)
        if tick + 1 < TICKS:
            passed = lax.ppermute(layer_out, "section", fwd)
            current = jnp.where(section_pos == 0, arriving[tick], passed)
    return jnp.stack(results)[None]


def solution(mesh):
    devices = mesh.devices
    n_sec = devices.shape[0]
    m = Mesh(devices.reshape(n_sec, 2, devices.shape[1] // 4, 2), ("section", "y", "z", "core"))
    ex = ("y", "z", "core")
    return jax.shard_map(
        shards,
        mesh=m,
        in_specs=(
            P("section", ex, None),
            P(None, ex, None),
            P("section", None),
            P("section", None, ex),
            P("section", None, ex),
            P("section", ex, None),
            P("section", None, ex, None),
            P("section", None, ex),
        ),
        out_specs=P("section", None, ex, None),
        check_vma=False,
    )
```

```python
import functools

import jax
import jax.numpy as jnp
from jax import lax
from jax.experimental import pallas as pl
from jax.experimental.pallas import tpu as pltpu
from jax.sharding import Mesh, PartitionSpec as P

EXP_WIN = 2
TICKS = 2
CAP = 20
VMEM_MIB = 52


def routing_tables(token_ids, share, experts):
    count = token_ids.shape[0]
    flat_ids = token_ids.reshape(-1)
    member = (flat_ids[:, None] == experts[None, :]).astype(jnp.int32)
    position = jnp.cumsum(member, axis=0) - 1
    slot_index = jnp.sum(position * member, axis=1)
    which = jnp.sum(member * jnp.arange(EXP_WIN)[None, :], axis=1)
    valid = jnp.sum(member, axis=1) > 0
    target = jnp.where(valid, which * CAP + slot_index, -1)
    placed = (target[:, None] == jnp.arange(EXP_WIN * CAP)[None, :]).astype(jnp.float32)
    placed = placed.reshape(count, 2, EXP_WIN * CAP)
    dispatch_table = jnp.sum(placed, axis=1).T.astype(jnp.bfloat16)
    combine_table = placed[:, 0] * share[:, None] + placed[:, 1] * (1.0 - share)[:, None]
    return dispatch_table, combine_table


def shift(x, axis, by):
    n = lax.axis_size(axis)
    return lax.ppermute(x, axis, [(i, (i + by) % n) for i in range(n)])


SPLIT = 2
LANES = 128
COL_BLOCKS = 4


def ring_shift(x, by):
    nz = lax.axis_size("z")
    pairs = [(2 * z + c, 2 * ((z + (by if c == 0 else -by)) % nz) + c) for z in range(nz) for c in range(2)]
    return lax.ppermute(x, ("z", "core"), pairs)


def ffn_kernel(*refs, count):
    chunks, (ga, ua, da, gb, ub, db, out) = refs[:count], refs[count:count + 7]
    gubuf, dbuf, x, hid, hid_t, gsem, usem, dsem = refs[count + 7:]
    blk = gubuf.shape[1] // 2
    units = da.shape[0]
    f32 = jnp.float32
    r = out.shape[0]
    def start_block(at):
        g, u = ((ga, ua), (gb, ub))[at // SPLIT]
        k = at % SPLIT
        pltpu.make_async_copy(g.at[pl.ds(k * blk, blk)], gubuf.at[at, pl.ds(0, blk)], gsem.at[at]).start()
        pltpu.make_async_copy(u.at[pl.ds(k * blk, blk)], gubuf.at[at, pl.ds(blk, blk)], usem.at[at]).start()

    start_block(0)
    start_block(1)
    cols = out.shape[1] // COL_BLOCKS

    def down_copy(i, n):
        at = pl.multiple_of(n * cols, cols)
        src = (da, db)[i].at[:, pl.ds(at, cols)]
        return pltpu.make_async_copy(src, dbuf.at[pl.ds(i * units, units), pl.ds(at, cols)], dsem.at[i, n])

    def start_down(n):
        down_copy(0, n).start()
        down_copy(1, n).start()

    at = 0
    for c in chunks:
        x[pl.ds(at, c.shape[0]), :] = c[...]
        at += c.shape[0]
    if at < x.shape[0]:
        x[pl.ds(at, x.shape[0] - at), :] = jnp.zeros((x.shape[0] - at, x.shape[1]), x.dtype)

    def hidden_block(j, carry):
        pltpu.make_async_copy(ga.at[pl.ds(0, blk)], gubuf.at[j, pl.ds(0, blk)], gsem.at[j]).wait()
        pltpu.make_async_copy(ua.at[pl.ds(0, blk)], gubuf.at[j, pl.ds(blk, blk)], usem.at[j]).wait()
        for at in range(2, 2 * SPLIT):
            pl.when(j == at - 2)(functools.partial(start_block, at))
        for n in range(COL_BLOCKS):
            pl.when(j == min(n + 1, 2 * SPLIT - 1))(functools.partial(start_down, n))
        v = lax.dot_general(gubuf[j], x[...], (((1,), (1,)), ((), ())), preferred_element_type=f32)
        gv, uv = v[:blk], v[blk:]
        hid[j] = (gv / (1.0 + jnp.exp(-gv)) * uv).astype(jnp.bfloat16)
        return carry

    lax.fori_loop(0, 2 * SPLIT, hidden_block, 0)
    hid_t[...] = hid[...].reshape(2 * units, x.shape[0]).T

    def out_block(n, carry):
        down_copy(0, n).wait()
        down_copy(1, n).wait()
        at = pl.multiple_of(n * cols, cols)
        v = jnp.dot(hid_t[:r], dbuf[:, pl.ds(at, cols)], preferred_element_type=f32)
        out[:, pl.ds(at, cols)] = v.astype(jnp.bfloat16)
        return carry

    lax.fori_loop(0, COL_BLOCKS, out_block, 0)


def ffn(chunks, weights):
    r, d = sum(c.shape[0] for c in chunks), chunks[0].shape[1]
    rp = -(-r // LANES) * LANES
    (ga, ua, da), (gb, ub, db) = weights
    units = da.shape[0]
    blk = units // SPLIT
    bf16 = jnp.bfloat16
    vmem, hbm = pl.BlockSpec(memory_space=pltpu.VMEM), pl.BlockSpec(memory_space=pltpu.HBM)
    return pl.pallas_call(
        functools.partial(ffn_kernel, count=len(chunks)),
        out_shape=jax.ShapeDtypeStruct((r, d), bf16),
        in_specs=[vmem] * len(chunks) + [hbm] * 6,
        out_specs=vmem,
        scratch_shapes=[
            pltpu.VMEM((2 * SPLIT, 2 * blk, d), bf16),
            pltpu.VMEM((2 * units, d), bf16),
            pltpu.VMEM((rp, d), bf16),
            pltpu.VMEM((2 * SPLIT, blk, rp), bf16),
            pltpu.VMEM((rp, 2 * units), bf16),
            pltpu.SemaphoreType.DMA((2 * SPLIT,)),
            pltpu.SemaphoreType.DMA((2 * SPLIT,)),
            pltpu.SemaphoreType.DMA((2, COL_BLOCKS)),
        ],
        cost_estimate=pl.CostEstimate(flops=12 * r * d * units, transcendentals=2 * r * units,
                                      bytes_accessed=12 * units * d + 4 * r * d),
        compiler_params=pltpu.CompilerParams(vmem_limit_bytes=VMEM_MIB * 1024 * 1024),
        name="ffn",
    )(*chunks, ga, ua, da, gb, ub, db)


def mixed_experts(block, weights):
    f32, bf16 = jnp.float32, jnp.bfloat16
    half = lax.axis_size("z") // 2
    n = block.shape[0]
    mine, other = [block], [shift(block, "core", 1)]
    for s in range(1, half):
        mine.append(ring_shift(mine[-1], 1))
        other.append(ring_shift(other[-1], 1))
    near = [block]
    for s in range(1, half - 1):
        near += [mine[s], other[s]]
    far_part = ffn([mine[-1], other[-1], ring_shift(mine[-1], 1)], weights)
    near[0], far_part = lax.optimization_barrier((block, far_part))
    near_part = ffn(near, weights)

    def part(s):
        if s == half - 1:
            return far_part[:n], far_part[n:2 * n]
        at = n * (2 * s - 1)
        return near_part[at:at + n], near_part[at + n:at + 2 * n]

    def after(x, first):
        return lax.optimization_barrier((x, first))[0]

    a, b = far_part[2 * n:], None
    for s in range(half - 1, 0, -1):
        pm, po = part(s)
        b = po if b is None else (po.astype(f32) + b).astype(bf16)
        sent, b = b, ring_shift(b, -1)
        a = after(ring_shift(a, -1), sent)
        a = (pm.astype(f32) + a).astype(bf16)
    c = shift(b, "core", 1)
    a = ring_shift(a, -1)
    return near_part[:n].astype(f32) + a + c


def shards(initial, arriving, gains, gate_w, up_w, down_w, pairs, shares):
    section_pos = lax.axis_index("section")
    y_pos = lax.axis_index("y")
    gain = gains[0]
    mine = (gate_w[0].T, up_w[0].T, down_w[0])
    weights = (mine, tuple(shift(w, "core", 1) for w in mine))
    current = initial[0]
    experts = jnp.stack([y_pos, 1 - y_pos]).astype(jnp.int32)
    swap = [(0, 1), (1, 0)]
    n_sec = lax.axis_size("section")
    fwd = [(i, i + 1) for i in range(n_sec - 1)]
    results = []
    for tick in range(TICKS):
        widened = current.astype(jnp.float32)
        scale = lax.rsqrt(jnp.mean(widened * widened, axis=-1, keepdims=True) + 1e-06)
        normed = (widened * scale * gain).astype(jnp.bfloat16)
        disp, comb = routing_tables(pairs[0, tick], shares[0, tick], experts)
        send_rows = jnp.dot(disp, normed, preferred_element_type=jnp.float32).astype(jnp.bfloat16)
        own, other = send_rows[:CAP], send_rows[CAP:]
        got = lax.ppermute(other, "y", swap)
        block = jnp.concatenate([own, got], axis=0)
        summed = mixed_experts(block, weights).astype(jnp.bfloat16)
        back = lax.ppermute(summed[CAP:], "y", swap)
        both = jnp.concatenate([summed[:CAP], back], axis=0)
        mixture = jnp.dot(comb, both.astype(jnp.float32), precision=lax.Precision.HIGHEST)
        mixture = mixture.astype(jnp.bfloat16)
        layer_out = (widened + mixture.astype(jnp.float32)).astype(jnp.bfloat16)
        results.append(layer_out)
        if tick + 1 < TICKS:
            passed = lax.ppermute(layer_out, "section", fwd)
            current = jnp.where(section_pos == 0, arriving[tick], passed)
    return jnp.stack(results)[None]


def solution(mesh):
    devices = mesh.devices
    n_sec = devices.shape[0]
    m = Mesh(devices.reshape(n_sec, 2, devices.shape[1] // 4, 2), ("section", "y", "z", "core"))
    ex = ("y", "z", "core")
    return jax.shard_map(
        shards,
        mesh=m,
        in_specs=(
            P("section", ex, None),
            P(None, ex, None),
            P("section", None),
            P("section", None, ex),
            P("section", None, ex),
            P("section", ex, None),
            P("section", None, ex, None),
            P("section", None, ex),
        ),
        out_specs=P("section", None, ex, None),
        check_vma=False,
    )
```

```python
import functools

import jax
import jax.numpy as jnp
from jax import lax
from jax.experimental import pallas as pl
from jax.experimental.pallas import tpu as pltpu
from jax.sharding import Mesh, PartitionSpec as P

EXP_WIN = 2
TICKS = 2
CAP = 20
VMEM_MIB = 52


def routing_tables(token_ids, share, experts):
    count = token_ids.shape[0]
    flat_ids = token_ids.reshape(-1)
    member = (flat_ids[:, None] == experts[None, :]).astype(jnp.int32)
    position = jnp.cumsum(member, axis=0) - 1
    slot_index = jnp.sum(position * member, axis=1)
    which = jnp.sum(member * jnp.arange(EXP_WIN)[None, :], axis=1)
    valid = jnp.sum(member, axis=1) > 0
    target = jnp.where(valid, which * CAP + slot_index, -1)
    placed = (target[:, None] == jnp.arange(EXP_WIN * CAP)[None, :]).astype(jnp.float32)
    placed = placed.reshape(count, 2, EXP_WIN * CAP)
    dispatch_table = jnp.sum(placed, axis=1).T.astype(jnp.bfloat16)
    combine_table = placed[:, 0] * share[:, None] + placed[:, 1] * (1.0 - share)[:, None]
    return dispatch_table, combine_table


def shift(x, axis, by):
    n = lax.axis_size(axis)
    return lax.ppermute(x, axis, [(i, (i + by) % n) for i in range(n)])


SPLIT = 2
LANES = 128
COL_BLOCKS = 4


def ring_shift(x, by):
    nz = lax.axis_size("z")
    pairs = [(2 * z + c, 2 * ((z + (by if c == 0 else -by)) % nz) + c) for z in range(nz) for c in range(2)]
    return lax.ppermute(x, ("z", "core"), pairs)


def ffn_kernel(*refs, count):
    chunks, (ga, ua, da, gb, ub, db, out) = refs[:count], refs[count:count + 7]
    gubuf, dbuf, x, hid, hid_t, gsem, usem, dsem = refs[count + 7:]
    blk = gubuf.shape[1] // 2
    units = da.shape[0]
    f32 = jnp.float32
    r = out.shape[0]
    def start_block(at):
        g, u = ((ga, ua), (gb, ub))[at // SPLIT]
        k = at % SPLIT
        pltpu.make_async_copy(g.at[pl.ds(k * blk, blk)], gubuf.at[at, pl.ds(0, blk)], gsem.at[at]).start()
        pltpu.make_async_copy(u.at[pl.ds(k * blk, blk)], gubuf.at[at, pl.ds(blk, blk)], usem.at[at]).start()

    start_block(0)
    start_block(1)
    cols = out.shape[1] // COL_BLOCKS

    def down_copy(i, n):
        at = pl.multiple_of(n * cols, cols)
        src = (da, db)[i].at[:, pl.ds(at, cols)]
        return pltpu.make_async_copy(src, dbuf.at[pl.ds(i * units, units), pl.ds(at, cols)], dsem.at[i, n])

    def start_down(n):
        down_copy(0, n).start()
        down_copy(1, n).start()

    at = 0
    for c in chunks:
        x[pl.ds(at, c.shape[0]), :] = c[...]
        at += c.shape[0]
    if at < x.shape[0]:
        x[pl.ds(at, x.shape[0] - at), :] = jnp.zeros((x.shape[0] - at, x.shape[1]), x.dtype)

    def hidden_block(j, carry):
        pltpu.make_async_copy(ga.at[pl.ds(0, blk)], gubuf.at[j, pl.ds(0, blk)], gsem.at[j]).wait()
        pltpu.make_async_copy(ua.at[pl.ds(0, blk)], gubuf.at[j, pl.ds(blk, blk)], usem.at[j]).wait()
        for at in range(2, 2 * SPLIT):
            pl.when(j == at - 2)(functools.partial(start_block, at))
        for n in range(COL_BLOCKS):
            pl.when(j == min(n + 1, 2 * SPLIT - 1))(functools.partial(start_down, n))
        v = lax.dot_general(gubuf[j], x[...], (((1,), (1,)), ((), ())), preferred_element_type=f32)
        gv, uv = v[:blk], v[blk:]
        hid[j] = (gv / (1.0 + jnp.exp(-gv)) * uv).astype(jnp.bfloat16)
        return carry

    lax.fori_loop(0, 2 * SPLIT, hidden_block, 0)
    hid_t[...] = hid[...].reshape(2 * units, x.shape[0]).T

    def out_block(n, carry):
        down_copy(0, n).wait()
        down_copy(1, n).wait()
        at = pl.multiple_of(n * cols, cols)
        v = jnp.dot(hid_t[:r], dbuf[:, pl.ds(at, cols)], preferred_element_type=f32)
        out[:, pl.ds(at, cols)] = v.astype(jnp.bfloat16)
        return carry

    lax.fori_loop(0, COL_BLOCKS, out_block, 0)


def ffn(chunks, weights):
    r, d = sum(c.shape[0] for c in chunks), chunks[0].shape[1]
    rp = -(-r // LANES) * LANES
    (ga, ua, da), (gb, ub, db) = weights
    units = da.shape[0]
    blk = units // SPLIT
    bf16 = jnp.bfloat16
    vmem, hbm = pl.BlockSpec(memory_space=pltpu.VMEM), pl.BlockSpec(memory_space=pltpu.HBM)
    return pl.pallas_call(
        functools.partial(ffn_kernel, count=len(chunks)),
        out_shape=jax.ShapeDtypeStruct((r, d), bf16),
        in_specs=[vmem] * len(chunks) + [hbm] * 6,
        out_specs=vmem,
        scratch_shapes=[
            pltpu.VMEM((2 * SPLIT, 2 * blk, d), bf16),
            pltpu.VMEM((2 * units, d), bf16),
            pltpu.VMEM((rp, d), bf16),
            pltpu.VMEM((2 * SPLIT, blk, rp), bf16),
            pltpu.VMEM((rp, 2 * units), bf16),
            pltpu.SemaphoreType.DMA((2 * SPLIT,)),
            pltpu.SemaphoreType.DMA((2 * SPLIT,)),
            pltpu.SemaphoreType.DMA((2, COL_BLOCKS)),
        ],
        cost_estimate=pl.CostEstimate(flops=12 * r * d * units, transcendentals=2 * r * units,
                                      bytes_accessed=12 * units * d + 4 * r * d),
        compiler_params=pltpu.CompilerParams(vmem_limit_bytes=VMEM_MIB * 1024 * 1024),
        name="ffn",
    )(*chunks, ga, ua, da, gb, ub, db)


def mixed_experts(block, weights):
    f32, bf16 = jnp.float32, jnp.bfloat16
    half = lax.axis_size("z") // 2
    n = block.shape[0]
    mine, other = [block], [shift(block, "core", 1)]
    for s in range(1, half):
        mine.append(ring_shift(mine[-1], 1))
        other.append(ring_shift(other[-1], 1))
    near = [block]
    for s in range(1, half - 1):
        near += [mine[s], other[s]]
    far_part = ffn([mine[-1], other[-1], ring_shift(mine[-1], 1)], weights)
    near[0], far_part = lax.optimization_barrier((block, far_part))
    near_part = ffn(near, weights)

    def part(s):
        if s == half - 1:
            return far_part[:n], far_part[n:2 * n]
        at = n * (2 * s - 1)
        return near_part[at:at + n], near_part[at + n:at + 2 * n]

    def after(x, first):
        return lax.optimization_barrier((x, first))[0]

    a, b = far_part[2 * n:], None
    for s in range(half - 1, 0, -1):
        pm, po = part(s)
        b = po if b is None else (po.astype(f32) + b).astype(bf16)
        sent, b = b, ring_shift(b, -1)
        a = after(ring_shift(a, -1), sent)
        a = (pm.astype(f32) + a).astype(bf16)
    c = shift(b, "core", 1)
    a = ring_shift(a, -1)
    return near_part[:n].astype(f32) + a + c


def combine(widened, comb, own, other):
    both = jnp.concatenate([own, other], axis=0).astype(jnp.float32)
    mixture = jnp.dot(comb, both, precision=lax.Precision.HIGHEST).astype(jnp.bfloat16)
    return (widened + mixture.astype(jnp.float32)).astype(jnp.bfloat16)


def shards(initial, arriving, gains, gate_w, up_w, down_w, pairs, shares):
    section_pos = lax.axis_index("section")
    y_pos = lax.axis_index("y")
    gain = gains[0]
    mine = (gate_w[0].T, up_w[0].T, down_w[0])
    weights = (mine, tuple(shift(w, "core", 1) for w in mine))
    current = initial[0]
    experts = jnp.stack([y_pos, 1 - y_pos]).astype(jnp.int32)
    swap = [(0, 1), (1, 0)]
    n_sec = lax.axis_size("section")
    fwd = [(i, i + 1) for i in range(n_sec - 1)]
    fwd_swap = [(2 * i + y, 2 * (i + 1) + 1 - y) for i in range(n_sec - 1) for y in range(2)]
    results = []
    for tick in range(TICKS):
        widened = current.astype(jnp.float32)
        scale = lax.rsqrt(jnp.mean(widened * widened, axis=-1, keepdims=True) + 1e-06)
        normed = (widened * scale * gain).astype(jnp.bfloat16)
        disp, comb = routing_tables(pairs[0, tick], shares[0, tick], experts)
        send_rows = jnp.dot(disp, normed, preferred_element_type=jnp.float32).astype(jnp.bfloat16)
        own, other = send_rows[:CAP], send_rows[CAP:]
        got = lax.ppermute(other, "y", swap)
        block = jnp.concatenate([own, got], axis=0)
        if tick + 1 < TICKS:
            ahead, comb_ahead = lax.optimization_barrier((lax.ppermute(current, "section", fwd), lax.ppermute(comb, "section", fwd)))
        summed = mixed_experts(block, weights).astype(jnp.bfloat16)
        ours, theirs = summed[:CAP], summed[CAP:]
        back = lax.ppermute(theirs, "y", swap)
        if tick + 1 < TICKS:
            ours_ahead = lax.ppermute(ours, "section", fwd)
            back_ahead = lax.ppermute(theirs, ("section", "y"), fwd_swap)
            passed = combine(ahead.astype(jnp.float32), comb_ahead, ours_ahead, back_ahead)
            current = jnp.where(section_pos == 0, arriving[tick], passed)
        results.append(combine(widened, comb, ours, back))
    return jnp.stack(results)[None]


def solution(mesh):
    devices = mesh.devices
    n_sec = devices.shape[0]
    m = Mesh(devices.reshape(n_sec, 2, devices.shape[1] // 4, 2), ("section", "y", "z", "core"))
    ex = ("y", "z", "core")
    return jax.shard_map(
        shards,
        mesh=m,
        in_specs=(
            P("section", ex, None),
            P(None, ex, None),
            P("section", None),
            P("section", None, ex),
            P("section", None, ex),
            P("section", ex, None),
            P("section", None, ex, None),
            P("section", None, ex),
        ),
        out_specs=P("section", None, ex, None),
        check_vma=False,
    )
```
